32 devices in a mesh: dp: 4 (over x, core), expert: 8 (over z, y).
Axes of the slice: x: 2, y: 2, z: 4, core: 2. Of those that a mesh axis runs over, the one named last changes fastest.
Arguments:
- tokens: bfloat16 [4096, 1024], P(('dp', 'expert')), may hold values from -6 to 6
- task_ids: int32 [32], P('dp'), may hold values from 0 to 5
- routing: int32 [32, 2], P('dp'), may hold values from 0 to 7, all different within a row; in each aligned block of 8 rows (0 to 7, 8 to 15, ...) at most 3 rows name the same one
- gate_weight: bfloat16 [1024, 48], replicated, may hold values from -0.1875 to 0.1875
- w_in: bfloat16 [8, 1024, 4096], P('expert', None, 'dp'), may hold values from -0.1875 to 0.1875
- w_out: bfloat16 [8, 4096, 1024], P('expert', 'dp'), may hold values from -0.09375 to 0.09375
Outputs:
- mixed: bfloat16 [4096, 1024], P(('dp', 'expert'))
The draws below stay inside these ranges and needn't reach their ends.
Inputs may be any that keep to these rules, and one draw needn't show every extreme that they name: `routing`: each row names two different experts. Within the 8 blocks of one index of dp no expert is named more than 3 times, a bound that some block reaches.
All inputs are finite; a program needn't handle non-finite values.
Results may differ from the reference program's by a relative error of at most 0.015.
Values may be sent and summed in bfloat16 or wider, within the bound.
No kernel may reach another device: no remote copies, remote signals or barrier semaphores. Data moves between devices by JAX's collectives and lax.ppermute only.
A program may use at most 64 MiB of HBM per device.

```python
import math
import jax
import jax.numpy as jnp
import numpy as np
from jax import lax

D = 1024
FF = 4096
TASKS = 6
BLK = 128
EXPERTS = 8
ROWBLK = 8
CAP = 3
BLOCKS = 32
TOKENS = 4096
N_DP = 4


def with_ends(array, stream_key, smallest, high):
    extent = array.shape
    index_at = [jax.random.randint(jax.random.fold_in(stream_key, axis), (), 0, extent[axis]) for axis in range(len(extent))]
    array = array.at[tuple(index_at)].set(smallest)
    longest = extent.index(max(extent))
    index_at[longest] = (index_at[longest] + 1) % extent[longest]
    return array.at[tuple(index_at)].set(high)


def level_of(stream_key, shape, shards, smallest, largest):
    def one(dim, blocks):
        draws = jax.random.uniform(jax.random.fold_in(jax.random.fold_in(stream_key, 6), dim), (blocks,), jnp.float32, smallest / len(shards), largest / len(shards))
        return jnp.repeat(jnp.exp(draws), shape[dim] // blocks).reshape((-1,) + (1,) * (len(shape) - dim - 1))

    loudness = one(*shards[0])
    for cut in shards[1:]:
        loudness = loudness * one(*cut)
    return loudness


def routed_block(key, own, number, rows, count, top, most, lean):
    sequence = jax.random.permutation(key, count)
    heavy_load, ordinary = load_shares(count, rows * top, most, lean, True), load_shares(count, rows * top, most, lean, False)
    places = jnp.arange(count)

    def named(tallies, offset_by):
        used = int((tallies > 0).sum())
        fixed = max(1, used // 4)
        shifted = fixed + (places - fixed + offset_by * (used - fixed)) % max(1, count - fixed)
        return jnp.zeros((count,), jnp.int32).at[sequence[jnp.where(places < fixed, places, shifted)]].set(jnp.asarray(tallies, jnp.int32))

    tallies = jnp.where(number % 4 == 0, named(heavy_load, number // 4), named(ordinary, number - number // 4 - 1))
    mixed = jax.random.permutation(jax.random.fold_in(own, 3), count)
    source_of, taker = mixed[0:count // 2 * 2:2], mixed[1:count // 2 * 2:2]
    slack = jnp.minimum(tallies[source_of] - 1, most - tallies[taker]) // 2
    slack = jnp.where((source_of == sequence[0]) | (taker == sequence[0]) | (tallies[taker] == 0), 0, jnp.maximum(slack, 0))
    shifted = jax.random.randint(jax.random.fold_in(own, 4), (count // 2,), 0, 1 << 20) % (slack + 1)
    tallies = tallies.at[source_of].add(-shifted).at[taker].add(shifted)
    members = jnp.searchsorted(jnp.cumsum(tallies), jnp.arange(rows * top), side="right").astype(jnp.int32)
    table = members.reshape(top, rows).T
    table = table[jax.random.permutation(jax.random.fold_in(own, 1), rows)]
    offset_by = jax.random.randint(jax.random.fold_in(own, 2), (rows, 1), 0, top)
    return jnp.take_along_axis(table, (jnp.arange(top)[None, :] + offset_by) % top, axis=1)


def load_shares(count, total, bound, slope, full):
    weights = [(1 << 20) // math.isqrt(grade ** slope) + 1 for grade in range(1, count + 1)]
    largest = bound if full else min(bound, max(-(-total // count), total * weights[0] // sum(weights)))
    least = 1 if total - largest >= count - 1 else 0
    given, surplus = [largest] + [least] * (count - 1), total - largest - least * (count - 1)
    while surplus > 0:
        candidates = [i for i in range(1, count) if given[i] < largest] or [i for i in range(1, count) if given[i] < bound]
        mass, left = sum([weights[i] for i in candidates]), surplus
        for i in candidates:
            addition = min(bound - given[i], max(1, left * weights[i] // mass), surplus)
            given[i] = given[i] + addition
            surplus = surplus - addition
    return np.array(given)


def bell_draw(stream_key, dims, width, most, shards=(), dtype=jnp.bfloat16):
    level = level_of(stream_key, dims, shards, -0.22, 0.18) if shards else 1.0
    entries = jax.random.normal(stream_key, dims, jnp.float32) * width * level
    return jnp.minimum(jnp.maximum(entries, -most), most).astype(dtype)


def setup_inputs(seed: int = 0) -> dict:
    splits = jax.random.split(jax.random.key(seed), 7)
    tokens = bell_draw(splits[0], (TOKENS, D), 1.0, 6.0, ((0, 32),))
    task_ids = with_ends(jax.random.randint(splits[1], (BLOCKS,), 0, TASKS), jax.random.fold_in(splits[1], 1), 0, TASKS - 1).astype(jnp.int32)
    routing_keys = jax.random.split(jax.random.fold_in(splits[2], 1), BLOCKS // ROWBLK)
    routing_turns = jax.random.permutation(jax.random.fold_in(splits[2], 3), BLOCKS // ROWBLK)
    routing = jax.vmap(lambda own, number: routed_block(jax.random.fold_in(splits[2], 2), own, number, ROWBLK, EXPERTS, 2, CAP, 2))(routing_keys, routing_turns).reshape((BLOCKS, 2))
    gate_weight = bell_draw(splits[3], (D, TASKS * EXPERTS), D ** -0.5, 0.1875)
    w_in = bell_draw(splits[4], (EXPERTS, D, FF), D ** -0.5, 0.1875, ((0, 8), (2, 4)))
    w_out = bell_draw(splits[5], (EXPERTS, FF, D), FF ** -0.5, 0.09375, ((0, 8), (1, 4)))
    return dict(tokens=tokens, task_ids=task_ids, routing=routing, gate_weight=gate_weight, w_in=w_in, w_out=w_out)


def expert_output(block_rows, expert_id, w_in, w_out):
    hidden = jax.nn.gelu(jnp.dot(block_rows, w_in[expert_id], preferred_element_type=jnp.float32)).astype(jnp.bfloat16)
    slice_width = FF // N_DP
    hidden_split = hidden.reshape(BLK, N_DP, slice_width).astype(jnp.float32)
    weight_split = w_out[expert_id].reshape(N_DP, slice_width, D).astype(jnp.float32)
    partials = jnp.einsum("bjs,jsd->jbd", hidden_split, weight_split).astype(jnp.bfloat16)
    partials = lax.optimization_barrier(partials).astype(jnp.float32)
    return jnp.sum(partials, axis=0)


def reference(tokens, task_ids, routing, gate_weight, w_in, w_out):
    token_blocks = tokens.reshape(BLOCKS, BLK, D)

    def per_block(inputs):
        block_rows, task_id, route_pair = inputs
        logits = jnp.dot(block_rows, gate_weight, preferred_element_type=jnp.float32).reshape(BLK, TASKS, EXPERTS)
        task_logits = lax.dynamic_index_in_dim(logits, task_id, 1, keepdims=False)
        logit_first = task_logits[:, route_pair[0]]
        logit_second = task_logits[:, route_pair[1]]
        gate_first = jax.nn.sigmoid(logit_first - logit_second)
        gate_second = jax.nn.sigmoid(logit_second - logit_first)
        first_sum = expert_output(block_rows, route_pair[0], w_in, w_out)
        second_sum = expert_output(block_rows, route_pair[1], w_in, w_out)
        gated_first = (gate_first[:, None] * first_sum).astype(jnp.bfloat16)
        gated_second = (gate_second[:, None] * second_sum).astype(jnp.bfloat16)
        return (gated_first.astype(jnp.float32) + gated_second.astype(jnp.float32)).astype(jnp.bfloat16)

    mixed = lax.map(per_block, (token_blocks, task_ids, routing))
    return mixed.reshape(TOKENS, D)
```

```python
import functools

import jax
import jax.numpy as jnp
from jax import lax
from jax.sharding import PartitionSpec as P

BLK = 128
STREAMS = 1
MAJOR = 4
CORES = 2


def xor_pairs(size, mask):
    return [(i, i ^ mask) for i in range(size)]


def shards(tokens, task_ids, routing, gate_weight, w_in, w_out):
    n_experts = lax.axis_size("expert")
    n_dp = lax.axis_size("dp")
    me = lax.axis_index("expert")
    major = min(MAJOR, n_experts)
    minor = n_experts // major
    chips = n_dp // CORES
    capacity = 2 * (tokens.shape[0] // BLK) + 1
    width = tokens.shape[1]
    rows = BLK // STREAMS
    move = lambda x, mask: lax.ppermute(x, "expert", xor_pairs(n_experts, mask))
    move_dp = lambda x, mask: lax.ppermute(x, "dp", xor_pairs(n_dp, mask))

    blocks = jnp.arange(n_experts, dtype=jnp.int32)
    slots = jnp.arange(capacity, dtype=jnp.int32)

    def slot_table(expert):
        chosen = jnp.any(routing == expert, axis=1)
        rank = jnp.sum((blocks[None, :] < blocks[:, None]) & chosen[None, :], axis=1)
        hit = chosen[None, :] & (rank[None, :] == slots[:, None])
        return hit

    hit = slot_table(me)
    hit_int = hit.astype(jnp.int32)
    home = jnp.sum(hit_int * blocks[None, :], axis=1)
    other = jnp.where(routing[:, 0] == me, routing[:, 1], routing[:, 0])
    slot_task = jnp.sum(hit_int * task_ids[None, :], axis=1)
    slot_other = jnp.sum(hit_int * other[None, :], axis=1)
    source = home ^ me

    columns = jnp.arange(gate_weight.shape[1], dtype=jnp.int32)
    pick_self = columns[None, :] == (slot_task * n_experts + me)[:, None]
    pick_other = columns[None, :] == (slot_task * n_experts + slot_other)[:, None]
    pick = pick_self.astype(jnp.float32) - pick_other.astype(jnp.float32)

    homes_from = []
    for kb in range(minor):
        table = slot_table(me ^ kb)
        homes_from.append(
            jnp.where(jnp.any(table, axis=1), jnp.sum(table * blocks[None, :], axis=1), -1)
        )

    weight_in, weight_out = w_in[0], w_out[0]

    def ffn(x):
        hidden = jax.nn.gelu(jnp.dot(x, weight_in, preferred_element_type=jnp.float32))
        return jnp.dot(
            hidden.astype(jnp.bfloat16), weight_out, preferred_element_type=jnp.float32
        ).astype(jnp.bfloat16)

    outs = []
    for stream in range(STREAMS):
        own = tokens[stream * rows : (stream + 1) * rows]
        gathered = {}
        for ka in reversed(range(major)):
            gathered[ka, 0] = own if ka == 0 else move(own, ka * minor)
        for ka in range(major):
            for kb in range(1, minor):
                gathered[ka, kb] = move(gathered[ka, 0], kb)
        picked = []
        for s in range(capacity):
            value = own
            for (ka, kb), block in gathered.items():
                value = jnp.where(source[s] == ka * minor + kb, block, value)
            picked.append(value)
        picked = jnp.concatenate(picked, axis=0)

        foreign = {0: picked}
        for chip in range(1, chips):
            foreign[chip * CORES] = move_dp(picked, chip * CORES)
        for chip in range(chips):
            foreign[chip * CORES + 1] = move_dp(foreign[chip * CORES], 1)

        logits = jnp.dot(picked, gate_weight, preferred_element_type=jnp.float32)
        logits = logits.reshape(capacity, rows, -1)
        gate = jax.nn.sigmoid(jnp.sum(logits * pick[:, None, :], axis=2))

        partial = {k: ffn(v) for k, v in foreign.items()}
        summed = {}
        for chip in range(chips):
            k = chip * CORES
            summed[k] = partial[k].astype(jnp.float32) + move_dp(partial[k + 1], 1).astype(
                jnp.float32
            )
        total = summed[0]
        for chip in range(1, chips):
            k = chip * CORES
            total = total + move_dp(summed[k].astype(jnp.bfloat16), k).astype(jnp.float32)
        gated = (gate[:, :, None] * total.reshape(capacity, rows, width)).astype(jnp.bfloat16)

        arrived = [gated] + [move(gated, kb) for kb in range(1, minor)]
        result = None
        for ka in reversed(range(major)):
            target = me ^ (ka * minor)
            value = jnp.zeros((rows, width), jnp.float32)
            for kb in range(minor):
                for s in range(capacity):
                    value = value + jnp.where(
                        homes_from[kb][s] == target, arrived[kb][s].astype(jnp.float32), 0.0
                    )
            if ka:
                value = move(value.astype(jnp.bfloat16), ka * minor).astype(jnp.float32)
            result = value if result is None else result + value
        outs.append(result.astype(jnp.bfloat16))
    return outs[0] if STREAMS == 1 else jnp.concatenate(outs, axis=0)


def solution(mesh):
    placed = (
        P(("dp", "expert"), None),
        P("dp"),
        P("dp", None),
        P(),
        P("expert", None, "dp"),
        P("expert", "dp", None),
    )
    return jax.shard_map(
        shards, mesh=mesh, in_specs=placed, out_specs=P(("dp", "expert"), None), check_vma=False
    )
```

```python
import functools
import math

import jax
import jax.numpy as jnp
from jax import lax
from jax.experimental import pallas as pl
from jax.experimental.pallas import tpu as pltpu
from jax.sharding import PartitionSpec as P


BLK = 128
STREAMS = 2
MAJOR = 4
CORES = 2
DIRECT = (0,1)
LANES = 128


VMEM = pl.BlockSpec(memory_space=pltpu.VMEM)
ANY = pl.BlockSpec(memory_space=pl.ANY)


def xor_pairs(size, mask):
    return [(i, i ^ mask) for i in range(size)]


def size_of(x):
    return math.prod(x.shape) * jnp.dtype(x.dtype).itemsize


def call(body, out_shapes, *operands, flops, in_specs=None, scratch=(), spare=4 * 2**20):
    moved = sum(size_of(x) for x in list(operands) + jax.tree.leaves(out_shapes))
    return pl.pallas_call(
        body,
        out_shape=out_shapes,
        in_specs=in_specs or [VMEM] * len(operands),
        out_specs=jax.tree.map(lambda _: VMEM, out_shapes),
        scratch_shapes=list(scratch),
        compiler_params=pltpu.CompilerParams(vmem_limit_bytes=moved + spare),
        cost_estimate=pl.CostEstimate(
            flops=int(flops), transcendentals=0, bytes_accessed=moved
        ),
    )(*operands)


def hold_body(n, *refs):
    copies = [pltpu.make_async_copy(refs[i], refs[n + i], refs[-1].at[i]) for i in range(n)]
    for copy in copies:
        copy.start()
    for copy in copies:
        copy.wait()


def add_body(a_ref, b_ref, out_ref):
    out_ref[...] = (a_ref[...].astype(jnp.float32) + b_ref[...].astype(jnp.float32)).astype(
        out_ref.dtype
    )


def combine_body(capacity, start, n, *refs):
    gate_ref, near, far, out_ref = refs[0], refs[1:3], refs[3 : 3 + n], refs[3 + n]
    rows = out_ref.shape[0] // capacity
    whole = near[0].shape[0] // capacity
    for s in range(capacity):
        cut, part = pl.ds(s * whole + start, rows), pl.ds(s * rows, rows)
        value = near[0][cut, :].astype(jnp.float32) + near[1][cut, :].astype(jnp.float32)
        for ref in far:
            value = value + ref[part, :].astype(jnp.float32)
        out_ref[part, :] = (value * gate_ref[cut, :][:, :1]).astype(out_ref.dtype)


def select_body(capacity, n, mask_ref, *refs):
    blocks, full_ref, outs, held, sems = refs[:n], refs[n], refs[n + 1 : -2], refs[-2], refs[-1]
    copies = [pltpu.make_async_copy(blocks[k], held.at[k], sems.at[k]) for k in range(1, n)]
    for copy in copies:
        copy.start()
    for copy in copies:
        copy.wait()
    rows = held.shape[1]
    part = rows // len(outs)
    for s in range(capacity):
        value = None
        for k in range(n):
            flag = mask_ref[pl.ds(s * n + k, 1), :][:, :1]
            term = (held[k] if k else blocks[0][...]) * flag
            value = term if value is None else value + term
        full_ref[pl.ds(s * rows, rows), :] = value
        for i, out_ref in enumerate(outs):
            out_ref[pl.ds(s * part, part), :] = value[i * part : (i + 1) * part]


def ffn_body(n, *refs):
    xs, w_in_ref, w_out_ref, outs = refs[:n], refs[n], refs[n + 1], refs[n + 2 :]
    for x_ref, out_ref in zip(xs, outs):
        hidden = jax.nn.gelu(
            jnp.dot(x_ref[...], w_in_ref[...], preferred_element_type=jnp.float32)
        ).astype(jnp.bfloat16)
        out_ref[...] = jnp.dot(
            hidden, w_out_ref[...], preferred_element_type=jnp.float32
        ).astype(jnp.bfloat16)


def gate_body(capacity, pick_ref, x_ref, gate_weight_ref, out_ref):
    rows = x_ref.shape[0] // capacity
    logits = jnp.dot(x_ref[...], gate_weight_ref[...], preferred_element_type=jnp.float32)
    for s in range(capacity):
        part = logits[s * rows : (s + 1) * rows] * pick_ref[pl.ds(s, 1), :]
        gate = jax.nn.sigmoid(jnp.sum(part, axis=1, keepdims=True))
        out_ref[pl.ds(s * rows, rows), :] = jnp.broadcast_to(gate, (rows, LANES))


def place_body(capacity, major, n, mask_ref, *refs):
    arrived, outs = refs[:n], refs[n:]
    rows = arrived[0].shape[0] // capacity
    step = min(rows, 16)

    @pl.loop(0, rows, step=step)
    def _(start):
        for ka in range(major):
            value = None
            for k in range(n):
                for s in range(capacity):
                    flag = mask_ref[pl.ds((ka * n + k) * capacity + s, 1), :][:, :1]
                    piece = arrived[k][pl.ds(s * rows + start, step), :]
                    term = piece.astype(jnp.float32) * flag
                    value = term if value is None else value + term
            outs[ka][pl.ds(start, step), :] = value.astype(outs[ka].dtype)


def shards(tokens, task_ids, routing, gate_weight, w_in, w_out):
    n_experts = lax.axis_size("expert")
    n_dp = lax.axis_size("dp")
    me = lax.axis_index("expert")
    major = min(MAJOR, n_experts)
    minor = n_experts // major
    chips = n_dp // CORES
    capacity = 2 * (tokens.shape[0] // BLK) + 1
    width = tokens.shape[1]
    rows = BLK // STREAMS
    move = lambda x, mask: lax.ppermute(x, "expert", xor_pairs(n_experts, mask))
    move_dp = lambda x, mask: lax.ppermute(x, "dp", xor_pairs(n_dp, mask))
    shape = lambda r, dtype=jnp.bfloat16: jax.ShapeDtypeStruct((r, width), dtype)

    blocks = jnp.arange(n_experts, dtype=jnp.int32)
    slots = jnp.arange(capacity, dtype=jnp.int32)

    experts = me ^ blocks[:minor]
    chosen = jnp.any(routing[None] == experts[:, None, None], axis=2)
    before = (blocks[None, :] < blocks[:, None])[None]
    rank = jnp.sum(before & chosen[:, None, :], axis=2)
    table = chosen[:, None, :] & (rank[:, None, :] == slots[None, :, None])
    hit = table[0].astype(jnp.int32)
    other = jnp.where(routing[:, 0] == me, routing[:, 1], routing[:, 0])
    slot_task = jnp.sum(hit * task_ids[None, :], axis=1)
    slot_other = jnp.sum(hit * other[None, :], axis=1)
    spread = lambda x: jnp.broadcast_to(x.reshape(-1, 1), (x.size, LANES))

    relative = (blocks[None, None, :] ^ me) == blocks[None, :, None]
    select_mask = spread(jnp.any(table[0][:, None, :] & relative, axis=2).astype(jnp.bfloat16))
    targets = me ^ (blocks[:major] * minor)
    place_mask = spread(
        jnp.any(
            table[None] & (blocks[None, None, None, :] == targets[:, None, None, None]), axis=3
        ).astype(jnp.float32)
    )
    columns = jnp.arange(gate_weight.shape[1], dtype=jnp.int32)
    pick_self = columns[None, :] == (slot_task * n_experts + me)[:, None]
    pick_other = columns[None, :] == (slot_task * n_experts + slot_other)[:, None]
    pick = pick_self.astype(jnp.float32) - pick_other.astype(jnp.float32)

    weight_in, weight_out = w_in[0], w_out[0]

    weight_in, weight_out, own_held = call(
        functools.partial(hold_body, 3),
        [jax.ShapeDtypeStruct(x.shape, x.dtype) for x in (weight_in, weight_out, tokens)],
        weight_in, weight_out, tokens,
        flops=1e8, in_specs=[ANY] * 3,
        scratch=[pltpu.SemaphoreType.DMA((3,))],
    )

    def ffn(xs):
        return call(
            functools.partial(ffn_body, len(xs)),
            [shape(x.shape[0]) for x in xs],
            *xs, weight_in, weight_out,
            spare=16 * 2**20,
            flops=4 * sum(x.size for x in xs) * weight_in.shape[1],
        )

    own = tokens
    gathered = {0: own}
    for mask in range(1, major):
        low = mask & -mask
        gathered[mask * minor] = move(gathered[(mask ^ low) * minor], low * minor)
    for ka in range(major):
        for kb in range(1, minor):
            gathered[ka * minor + kb] = move(gathered[ka * minor], kb)
    picked, *parts = call(
        functools.partial(select_body, capacity, n_experts),
        [shape(capacity * BLK)] + [shape(capacity * rows)] * STREAMS,
        select_mask, own_held, *[gathered[k] for k in range(1, n_experts)],
        spare=8 * 2**20, flops=2e8,
        in_specs=[VMEM] * 2 + [ANY] * (n_experts - 1),
        scratch=[
            pltpu.VMEM((n_experts, BLK, width), jnp.bfloat16),
            pltpu.SemaphoreType.DMA((n_experts,)),
        ],
    )

    foreign = []
    for part in parts:
        foreign.append({c: move_dp(part, c * CORES) for c in range(1, chips)})
    near = move_dp(picked, 1)
    gate = call(
        functools.partial(gate_body, capacity),
        jax.ShapeDtypeStruct((capacity * BLK, LANES), jnp.float32),
        pick, picked, gate_weight,
        flops=1e8,
    )
    mine, theirs = ffn([picked, near])
    theirs = move_dp(theirs, 1)

    outs = []
    for stream in range(STREAMS):
        backs = []
        for chip in range(1, chips):
            far = foreign[stream][chip]
            far_near = move_dp(far, 1)
            (kept,) = ffn([far])
            (sent,) = ffn([far_near])
            sent = move_dp(sent, 1)
            summed = call(add_body, shape(capacity * rows), kept, sent, flops=1e8)
            backs.append(move_dp(summed, chip * CORES))
        gated = call(
            functools.partial(combine_body, capacity, stream * rows, len(backs)),
            shape(capacity * rows),
            gate, mine, theirs, *backs,
            flops=1e8,
        )

        arrived = [gated] + [move(gated, kb) for kb in range(1, minor)]
        values = call(
            functools.partial(place_body, capacity, major, minor),
            [shape(rows)] * major,
            place_mask, *arrived,
            flops=1e8,
        )
        values = [v.astype(jnp.float32) for v in values]
        for mask in reversed(range(1, major)):
            low = mask if stream in DIRECT else mask & -mask
            back = move(values[mask].astype(jnp.bfloat16), low * minor)
            values[mask ^ low] = values[mask ^ low] + back.astype(jnp.float32)
        outs.append(values[0].astype(jnp.bfloat16))
    return outs[0] if STREAMS == 1 else jnp.concatenate(outs, axis=0)


def solution(mesh):
    placed = (
        P(("dp", "expert"), None),
        P("dp"),
        P("dp", None),
        P(),
        P("expert", None, "dp"),
        P("expert", "dp", None),
    )
    return jax.shard_map(
        shards, mesh=mesh, in_specs=placed, out_specs=P(("dp", "expert"), None), check_vma=False
    )
```

```python
import functools
import math

import jax
import jax.numpy as jnp
from jax import lax
from jax.experimental import pallas as pl
from jax.experimental.pallas import tpu as pltpu
from jax.sharding import PartitionSpec as P


BLK = 128
SPLIT = (4, 4)
MAJOR = 4
CORES = 2
SPLIT_SPARE = 4
SELECT_SPARE = 8
LANES = 128


VMEM = pl.BlockSpec(memory_space=pltpu.VMEM)
ANY = pl.BlockSpec(memory_space=pl.ANY)


def xor_pairs(size, mask):
    return [(i, i ^ mask) for i in range(size)]


def size_of(x):
    return math.prod(x.shape) * jnp.dtype(x.dtype).itemsize


def call(body, out_shapes, *operands, flops, in_specs=None, scratch=(), spare=4 * 2**20):
    moved = sum(size_of(x) for x in list(operands) + jax.tree.leaves(out_shapes))
    return pl.pallas_call(
        body,
        out_shape=out_shapes,
        in_specs=in_specs or [VMEM] * len(operands),
        out_specs=jax.tree.map(lambda _: VMEM, out_shapes),
        scratch_shapes=list(scratch),
        compiler_params=pltpu.CompilerParams(vmem_limit_bytes=moved + spare),
        cost_estimate=pl.CostEstimate(
            flops=int(flops), transcendentals=0, bytes_accessed=moved
        ),
    )(*operands)


def add_body(a_ref, b_ref, out_ref):
    out_ref[...] = (a_ref[...].astype(jnp.float32) + b_ref[...].astype(jnp.float32)).astype(
        out_ref.dtype
    )


def combine_body(*refs):
    gate_ref, parts, out_ref = refs[0], refs[1:-1], refs[-1]
    value = parts[0][...].astype(jnp.float32)
    for ref in parts[1:]:
        value = value + ref[...].astype(jnp.float32)
    out_ref[...] = (value * gate_ref[...][:, :1]).astype(out_ref.dtype)


def split_body(n, *refs):
    start, copies = 0, []
    for i in range(n):
        source = refs[0].at[pl.ds(start, refs[1 + i].shape[0]), :]
        copies.append(pltpu.make_async_copy(source, refs[1 + i], refs[-1].at[i]))
        start += refs[1 + i].shape[0]
    for copy in copies:
        copy.start()
    for copy in copies:
        copy.wait()


def select_body(capacity, n, mask_ref, *refs):
    blocks, out_ref, held, sems = refs[:n], refs[n], refs[n + 1], refs[n + 2]
    copies = [pltpu.make_async_copy(blocks[k], held.at[k], sems.at[k]) for k in range(1, n)]
    for copy in copies:
        copy.start()
    rows = held.shape[1]
    for k in range(n):
        if k:
            copies[k - 1].wait()
        for s in range(capacity):
            flag = mask_ref[pl.ds(s * n + k, 1), :][:, :1]
            term = (held[k] if k else blocks[0][...]) * flag
            part = pl.ds(s * rows, rows)
            out_ref[part, :] = out_ref[part, :] + term if k else term


def ffn_body(n, *refs):
    xs, w_in_ref, w_out_ref, outs = refs[:n], refs[n], refs[n + 1], refs[n + 2 :]
    for x_ref, out_ref in zip(xs, outs):
        hidden = jax.nn.gelu(
            jnp.dot(x_ref[...], w_in_ref[...], preferred_element_type=jnp.float32)
        ).astype(jnp.bfloat16)
        out_ref[...] = jnp.dot(
            hidden, w_out_ref[...], preferred_element_type=jnp.float32
        ).astype(jnp.bfloat16)


def gate_body(capacity, pick_ref, x_ref, gate_weight_ref, out_ref):
    rows = x_ref.shape[0] // capacity
    logits = lax.dot_general(
        x_ref[...], gate_weight_ref[...], (((1,), (1,)), ((), ())),
        preferred_element_type=jnp.float32,
    )
    for s in range(capacity):
        part = logits[s * rows : (s + 1) * rows] * pick_ref[pl.ds(s, 1), :]
        gate = jax.nn.sigmoid(jnp.sum(part, axis=1, keepdims=True))
        out_ref[pl.ds(s * rows, rows), :] = jnp.broadcast_to(gate, (rows, LANES))


def place_body(capacity, major, n, mask_ref, *refs):
    arrived, outs = refs[:n], refs[n:]
    rows = arrived[0].shape[0] // capacity
    step = min(rows, 16)

    @pl.loop(0, rows, step=step)
    def _(start):
        for ka in range(major):
            value = None
            for k in range(n):
                for s in range(capacity):
                    flag = mask_ref[pl.ds((ka * n + k) * capacity + s, 1), :][:, :1]
                    piece = arrived[k][pl.ds(s * rows + start, step), :]
                    term = piece.astype(jnp.float32) * flag
                    value = term if value is None else value + term
            outs[ka][pl.ds(start, step), :] = value.astype(outs[ka].dtype)


def shards(tokens, task_ids, routing, gate_weight, w_in, w_out):
    n_experts = lax.axis_size("expert")
    n_dp = lax.axis_size("dp")
    me = lax.axis_index("expert")
    major = min(MAJOR, n_experts)
    minor = n_experts // major
    chips = n_dp // CORES
    capacity = 2 * (tokens.shape[0] // BLK) + 1
    width = tokens.shape[1]
    split = [BLK * part // sum(SPLIT) for part in SPLIT]
    move = lambda x, mask: lax.ppermute(x, "expert", xor_pairs(n_experts, mask))
    move_dp = lambda x, mask: lax.ppermute(x, "dp", xor_pairs(n_dp, mask))
    shape = lambda r, dtype=jnp.bfloat16: jax.ShapeDtypeStruct((r, width), dtype)

    blocks = jnp.arange(n_experts, dtype=jnp.int32)
    slots = jnp.arange(capacity, dtype=jnp.int32)

    experts = me ^ blocks[:minor]
    chosen = jnp.any(routing[None] == experts[:, None, None], axis=2)
    before = (blocks[None, :] < blocks[:, None])[None]
    rank = jnp.sum(before & chosen[:, None, :], axis=2)
    table = chosen[:, None, :] & (rank[:, None, :] == slots[None, :, None])
    hit = table[0].astype(jnp.int32)
    other = jnp.where(routing[:, 0] == me, routing[:, 1], routing[:, 0])
    slot_task = jnp.sum(hit * task_ids[None, :], axis=1)
    slot_other = jnp.sum(hit * other[None, :], axis=1)
    spread = lambda x: jnp.broadcast_to(x.reshape(-1, 1), (x.size, LANES))

    relative = (blocks[None, None, :] ^ me) == blocks[None, :, None]
    select_mask = spread(jnp.any(table[0][:, None, :] & relative, axis=2).astype(jnp.bfloat16))
    targets = me ^ (blocks[:major] * minor)
    place_mask = spread(
        jnp.any(
            table[None] & (blocks[None, None, None, :] == targets[:, None, None, None]), axis=3
        ).astype(jnp.float32)
    )
    columns = jnp.arange(gate_weight.shape[1], dtype=jnp.int32)
    pick_self = columns[None, :] == (slot_task * n_experts + me)[:, None]
    pick_other = columns[None, :] == (slot_task * n_experts + slot_other)[:, None]
    pick = pick_self.astype(jnp.float32) - pick_other.astype(jnp.float32)

    weight_in, weight_out = w_in[0], w_out[0]

    def ffn(xs):
        return call(
            functools.partial(ffn_body, len(xs)),
            [shape(x.shape[0]) for x in xs],
            *xs, weight_in, weight_out,
            spare=16 * 2**20,
            flops=4 * sum(x.size for x in xs) * weight_in.shape[1],
        )

    owns = call(
        functools.partial(split_body, len(split)),
        [shape(rows) for rows in split],
        tokens,
        flops=1e8, in_specs=[ANY], spare=SPLIT_SPARE * 2**20,
        scratch=[pltpu.SemaphoreType.DMA((len(split),))],
    )
    outs = []
    for own, rows in zip(owns, split):
        full = shape(capacity * rows)

        gathered = {0: own}
        for mask in range(1, major):
            low = mask & -mask
            gathered[mask * minor] = move(gathered[(mask ^ low) * minor], low * minor)
        for ka in range(major):
            for kb in range(1, minor):
                gathered[ka * minor + kb] = move(gathered[ka * minor], kb)
        picked = call(
            functools.partial(select_body, capacity, n_experts),
            full,
            select_mask, *[gathered[k] for k in range(n_experts)],
            flops=2e8, spare=SELECT_SPARE * 2**20,
            in_specs=[VMEM] * 2 + [ANY] * (n_experts - 1),
            scratch=[
                pltpu.VMEM((n_experts, rows, width), jnp.bfloat16),
                pltpu.SemaphoreType.DMA((n_experts,)),
            ],
        )

        foreign = {chip: move_dp(picked, chip * CORES) for chip in range(1, chips)}
        near = move_dp(picked, 1)
        gate = call(
            functools.partial(gate_body, capacity),
            jax.ShapeDtypeStruct((capacity * rows, LANES), jnp.float32),
            pick, picked, gate_weight.T,
            flops=1e8,
        )
        mine, theirs = ffn([picked, near])
        theirs = move_dp(theirs, 1)
        backs = []
        for chip in range(1, chips):
            far = foreign[chip]
            far_near = move_dp(far, 1)
            (kept,) = ffn([far])
            (sent,) = ffn([far_near])
            sent = move_dp(sent, 1)
            summed = call(add_body, full, kept, sent, flops=1e8)
            backs.append(move_dp(summed, chip * CORES))
        gated = call(combine_body, full, gate, mine, theirs, *backs, flops=1e8)

        arrived = [gated] + [move(gated, kb) for kb in range(1, minor)]
        values = call(
            functools.partial(place_body, capacity, major, minor),
            [shape(rows)] * major,
            place_mask, *arrived,
            flops=1e8,
        )
        result = values[0].astype(jnp.float32)
        for mask in reversed(range(1, major)):
            result = result + move(values[mask], mask * minor).astype(jnp.float32)
        outs.append(result.astype(jnp.bfloat16))
    return jnp.concatenate(outs, axis=0)


def solution(mesh):
    placed = (
        P(("dp", "expert"), None),
        P("dp"),
        P("dp", None),
        P(),
        P("expert", None, "dp"),
        P("expert", "dp", None),
    )
    return jax.shard_map(
        shards, mesh=mesh, in_specs=placed, out_specs=P(("dp", "expert"), None), check_vma=False
    )
```

```python
import functools
import math

import jax
import jax.numpy as jnp
from jax import lax
from jax.experimental import pallas as pl
from jax.experimental.pallas import tpu as pltpu
from jax.sharding import PartitionSpec as P


BLK = 128
SPLIT = (4, 4)
MAJOR = 4
CORES = 2
SPLIT_SPARE = 4
LANES = 128
DIRECT = (0,)


VMEM = pl.BlockSpec(memory_space=pltpu.VMEM)
ANY = pl.BlockSpec(memory_space=pl.ANY)


def xor_pairs(size, mask):
    return [(i, i ^ mask) for i in range(size)]


def size_of(x):
    return math.prod(x.shape) * jnp.dtype(x.dtype).itemsize


def call(body, out_shapes, *operands, flops, in_specs=None, scratch=(), spare=4 * 2**20):
    moved = sum(size_of(x) for x in list(operands) + jax.tree.leaves(out_shapes))
    return pl.pallas_call(
        body,
        out_shape=out_shapes,
        in_specs=in_specs or [VMEM] * len(operands),
        out_specs=jax.tree.map(lambda _: VMEM, out_shapes),
        scratch_shapes=list(scratch),
        compiler_params=pltpu.CompilerParams(vmem_limit_bytes=moved + spare),
        cost_estimate=pl.CostEstimate(
            flops=int(flops), transcendentals=0, bytes_accessed=moved
        ),
    )(*operands)


def add_body(a_ref, b_ref, out_ref):
    out_ref[...] = (a_ref[...].astype(jnp.float32) + b_ref[...].astype(jnp.float32)).astype(
        out_ref.dtype
    )


def combine_body(*refs):
    gate_ref, parts, out_ref = refs[0], refs[1:-1], refs[-1]
    value = parts[0][...].astype(jnp.float32)
    for ref in parts[1:]:
        value = value + ref[...].astype(jnp.float32)
    out_ref[...] = (value * gate_ref[...][:, :1]).astype(out_ref.dtype)


def split_body(n, *refs):
    start, copies = 0, []
    for i in range(n):
        source = refs[0].at[pl.ds(start, refs[1 + i].shape[0]), :]
        copies.append(pltpu.make_async_copy(source, refs[1 + i], refs[-1].at[i]))
        start += refs[1 + i].shape[0]
    for copy in copies:
        copy.start()
    for copy in copies:
        copy.wait()


def select_body(capacity, n, source_ref, *refs):
    blocks, out_ref, sems = refs[:n], refs[n], refs[n + 1]
    rows = blocks[0].shape[0]
    for s in range(capacity):
        source = jnp.max(source_ref[pl.ds(s, 1), :])
        for k in range(n):

            @pl.when(source == k)
            def _():
                pltpu.make_async_copy(
                    blocks[k], out_ref.at[pl.ds(s * rows, rows), :], sems.at[s]
                ).start()

    for s in range(capacity):
        pltpu.make_async_copy(
            blocks[0], out_ref.at[pl.ds(s * rows, rows), :], sems.at[s]
        ).wait()


def ffn_body(n, *refs):
    xs, w_in_ref, w_out_ref, outs = refs[:n], refs[n], refs[n + 1], refs[n + 2 :]
    for x_ref, out_ref in zip(xs, outs):
        hidden = jax.nn.gelu(
            jnp.dot(x_ref[...], w_in_ref[...], preferred_element_type=jnp.float32)
        ).astype(jnp.bfloat16)
        out_ref[...] = jnp.dot(
            hidden, w_out_ref[...], preferred_element_type=jnp.float32
        ).astype(jnp.bfloat16)


def gate_body(capacity, pick_ref, x_ref, gate_weight_ref, out_ref):
    rows = x_ref.shape[0] // capacity
    logits = lax.dot_general(
        x_ref[...], gate_weight_ref[...], (((1,), (1,)), ((), ())),
        preferred_element_type=jnp.float32,
    )
    for s in range(capacity):
        part = logits[s * rows : (s + 1) * rows] * pick_ref[pl.ds(s, 1), :]
        gate = jax.nn.sigmoid(jnp.sum(part, axis=1, keepdims=True))
        out_ref[pl.ds(s * rows, rows), :] = jnp.broadcast_to(gate, (rows, LANES))


def place_body(capacity, major, n, mask_ref, *refs):
    arrived, outs = refs[:n], refs[n:]
    rows = arrived[0].shape[0] // capacity
    step = min(rows, 16)

    @pl.loop(0, rows, step=step)
    def _(start):
        for ka in range(major):
            value = None
            for k in range(n):
                for s in range(capacity):
                    flag = mask_ref[pl.ds((ka * n + k) * capacity + s, 1), :][:, :1]
                    piece = arrived[k][pl.ds(s * rows + start, step), :]
                    term = piece * flag
                    value = term if value is None else value + term
            outs[ka][pl.ds(start, step), :] = value.astype(outs[ka].dtype)


def shards(tokens, task_ids, routing, gate_weight, w_in, w_out):
    n_experts = lax.axis_size("expert")
    n_dp = lax.axis_size("dp")
    me = lax.axis_index("expert")
    major = min(MAJOR, n_experts)
    minor = n_experts // major
    chips = n_dp // CORES
    capacity = 2 * (tokens.shape[0] // BLK) + 1
    width = tokens.shape[1]
    split = [BLK * part // sum(SPLIT) for part in SPLIT]
    move = lambda x, mask: lax.ppermute(x, "expert", xor_pairs(n_experts, mask))
    move_dp = lambda x, mask: lax.ppermute(x, "dp", xor_pairs(n_dp, mask))
    shape = lambda r, dtype=jnp.bfloat16: jax.ShapeDtypeStruct((r, width), dtype)

    blocks = jnp.arange(n_experts, dtype=jnp.int32)
    slots = jnp.arange(capacity, dtype=jnp.int32)

    experts = me ^ blocks[:minor]
    chosen = jnp.any(routing[None] == experts[:, None, None], axis=2)
    before = (blocks[None, :] < blocks[:, None])[None]
    rank = jnp.sum(before & chosen[:, None, :], axis=2)
    table = chosen[:, None, :] & (rank[:, None, :] == slots[None, :, None])
    hit = table[0].astype(jnp.int32)
    other = jnp.where(routing[:, 0] == me, routing[:, 1], routing[:, 0])
    home = jnp.sum(hit * blocks[None, :], axis=1)
    slot_task = jnp.sum(hit * task_ids[None, :], axis=1)
    slot_other = jnp.sum(hit * other[None, :], axis=1)
    spread = lambda x: jnp.broadcast_to(x.reshape(-1, 1), (x.size, LANES))

    source = spread((home ^ me).astype(jnp.float32))
    targets = me ^ (blocks[:major] * minor)
    place_mask = spread(
        jnp.any(
            table[None] & (blocks[None, None, None, :] == targets[:, None, None, None]), axis=3
        ).astype(jnp.bfloat16)
    )
    columns = jnp.arange(gate_weight.shape[1], dtype=jnp.int32)
    pick_self = columns[None, :] == (slot_task * n_experts + me)[:, None]
    pick_other = columns[None, :] == (slot_task * n_experts + slot_other)[:, None]
    pick = pick_self.astype(jnp.float32) - pick_other.astype(jnp.float32)

    weight_in, weight_out = w_in[0], w_out[0]

    def ffn(xs):
        return call(
            functools.partial(ffn_body, len(xs)),
            [shape(x.shape[0]) for x in xs],
            *xs, weight_in, weight_out,
            spare=16 * 2**20,
            flops=4 * sum(x.size for x in xs) * weight_in.shape[1],
        )

    owns = call(
        functools.partial(split_body, len(split)),
        [shape(rows) for rows in split],
        tokens,
        flops=1e8, in_specs=[ANY], spare=SPLIT_SPARE * 2**20,
        scratch=[pltpu.SemaphoreType.DMA((len(split),))],
    )
    outs = []
    for stream, (own, rows) in enumerate(zip(owns, split)):
        full = shape(capacity * rows)

        gathered = {0: own}
        for mask in range(1, major):
            low = mask if stream in DIRECT else mask & -mask
            gathered[mask * minor] = move(gathered[(mask ^ low) * minor], low * minor)
        for ka in range(major):
            for kb in range(1, minor):
                gathered[ka * minor + kb] = move(gathered[ka * minor], kb)
        picked = call(
            functools.partial(select_body, capacity, n_experts),
            full,
            source, *[gathered[k] for k in range(n_experts)],
            flops=2e8,
            in_specs=[VMEM] + [ANY] * n_experts,
            scratch=[pltpu.SemaphoreType.DMA((capacity,))],
        )

        foreign = {chip: move_dp(picked, chip * CORES) for chip in range(1, chips)}
        near = move_dp(picked, 1)
        gate = call(
            functools.partial(gate_body, capacity),
            jax.ShapeDtypeStruct((capacity * rows, LANES), jnp.float32),
            pick, picked, gate_weight.T,
            flops=1e8,
        )
        mine, theirs = ffn([picked, near])
        theirs = move_dp(theirs, 1)
        backs = []
        for chip in range(1, chips):
            far = foreign[chip]
            far_near = move_dp(far, 1)
            (kept,) = ffn([far])
            (sent,) = ffn([far_near])
            sent = move_dp(sent, 1)
            summed = call(add_body, full, kept, sent, flops=1e8)
            backs.append(move_dp(summed, chip * CORES))
        gated = call(combine_body, full, gate, mine, theirs, *backs, flops=1e8)

        arrived = [gated] + [move(gated, kb) for kb in range(1, minor)]
        values = call(
            functools.partial(place_body, capacity, major, minor),
            [shape(rows)] * major,
            place_mask, *arrived,
            flops=1e8,
        )
        result = values[0].astype(jnp.float32)
        for mask in reversed(range(1, major)):
            result = result + move(values[mask], mask * minor).astype(jnp.float32)
        outs.append(result.astype(jnp.bfloat16))
    return jnp.concatenate(outs, axis=0)


def solution(mesh):
    placed = (
        P(("dp", "expert"), None),
        P("dp"),
        P("dp", None),
        P(),
        P("expert", None, "dp"),
        P("expert", "dp", None),
    )
    return jax.shard_map(
        shards, mesh=mesh, in_specs=placed, out_specs=P(("dp", "expert"), None), check_vma=False
    )
```

```python
import functools
import math

import jax
import jax.numpy as jnp
from jax import lax
from jax.experimental import pallas as pl
from jax.experimental.pallas import tpu as pltpu
from jax.sharding import PartitionSpec as P


BLK = 128
SPLIT = (4, 4)
MAJOR = 4
CORES = 2
LANES = 128
DIRECT = (0,)


VMEM = pl.BlockSpec(memory_space=pltpu.VMEM)
ANY = pl.BlockSpec(memory_space=pl.ANY)


def xor_pairs(size, mask):
    return [(i, i ^ mask) for i in range(size)]


def size_of(x):
    return math.prod(x.shape) * jnp.dtype(x.dtype).itemsize


def call(body, out_shapes, *operands, flops, in_specs=None, scratch=(), spare=4 * 2**20):
    moved = sum(size_of(x) for x in list(operands) + jax.tree.leaves(out_shapes))
    return pl.pallas_call(
        body,
        out_shape=out_shapes,
        in_specs=in_specs or [VMEM] * len(operands),
        out_specs=jax.tree.map(lambda _: VMEM, out_shapes),
        scratch_shapes=list(scratch),
        compiler_params=pltpu.CompilerParams(vmem_limit_bytes=moved + spare),
        cost_estimate=pl.CostEstimate(
            flops=int(flops), transcendentals=0, bytes_accessed=moved
        ),
    )(*operands)


def add_body(a_ref, b_ref, out_ref):
    out_ref[...] = (a_ref[...].astype(jnp.float32) + b_ref[...].astype(jnp.float32)).astype(
        out_ref.dtype
    )


def combine_body(*refs):
    gate_ref, parts, out_ref = refs[0], refs[1:-1], refs[-1]
    value = parts[0][...].astype(jnp.float32)
    for ref in parts[1:]:
        value = value + ref[...].astype(jnp.float32)
    out_ref[...] = (value * gate_ref[...][:, :1]).astype(out_ref.dtype)


def select_body(capacity, n, source_ref, *refs):
    blocks, out_ref, sems = refs[:n], refs[n], refs[n + 1]
    rows = blocks[0].shape[0]
    for s in range(capacity):
        source = jnp.max(source_ref[pl.ds(s, 1), :])
        for k in range(n):

            @pl.when(source == k)
            def _():
                pltpu.make_async_copy(
                    blocks[k], out_ref.at[pl.ds(s * rows, rows), :], sems.at[s]
                ).start()

    for s in range(capacity):
        pltpu.make_async_copy(
            blocks[0], out_ref.at[pl.ds(s * rows, rows), :], sems.at[s]
        ).wait()


def ffn_body(n, *refs):
    xs, w_in_ref, w_out_ref, outs = refs[:n], refs[n], refs[n + 1], refs[n + 2 :]
    for x_ref, out_ref in zip(xs, outs):
        hidden = jax.nn.gelu(
            jnp.dot(x_ref[...], w_in_ref[...], preferred_element_type=jnp.float32)
        ).astype(jnp.bfloat16)
        out_ref[...] = jnp.dot(
            hidden, w_out_ref[...], preferred_element_type=jnp.float32
        ).astype(jnp.bfloat16)


def gate_body(capacity, pick_ref, x_ref, gate_weight_ref, out_ref):
    rows = x_ref.shape[0] // capacity
    logits = lax.dot_general(
        x_ref[...], gate_weight_ref[...], (((1,), (1,)), ((), ())),
        preferred_element_type=jnp.float32,
    )
    for s in range(capacity):
        part = logits[s * rows : (s + 1) * rows] * pick_ref[pl.ds(s, 1), :]
        gate = jax.nn.sigmoid(jnp.sum(part, axis=1, keepdims=True))
        out_ref[pl.ds(s * rows, rows), :] = jnp.broadcast_to(gate, (rows, LANES))


def place_body(capacity, major, n, mask_ref, *refs):
    arrived, outs = refs[:n], refs[n:]
    rows = arrived[0].shape[0] // capacity
    step = min(rows, 16)

    @pl.loop(0, rows, step=step)
    def _(start):
        for ka in range(major):
            value = None
            for k in range(n):
                for s in range(capacity):
                    flag = mask_ref[pl.ds((ka * n + k) * capacity + s, 1), :][:, :1]
                    piece = arrived[k][pl.ds(s * rows + start, step), :]
                    term = piece * flag
                    value = term if value is None else value + term
            outs[ka][pl.ds(start, step), :] = value.astype(outs[ka].dtype)


def shards(tokens, task_ids, routing, gate_weight, w_in, w_out):
    n_experts = lax.axis_size("expert")
    n_dp = lax.axis_size("dp")
    me = lax.axis_index("expert")
    major = min(MAJOR, n_experts)
    minor = n_experts // major
    chips = n_dp // CORES
    capacity = 2 * (tokens.shape[0] // BLK) + 1
    width = tokens.shape[1]
    split = [BLK * part // sum(SPLIT) for part in SPLIT]
    move = lambda x, mask: lax.ppermute(x, "expert", xor_pairs(n_experts, mask))
    move_dp = lambda x, mask: lax.ppermute(x, "dp", xor_pairs(n_dp, mask))
    shape = lambda r, dtype=jnp.bfloat16: jax.ShapeDtypeStruct((r, width), dtype)

    blocks = jnp.arange(n_experts, dtype=jnp.int32)
    slots = jnp.arange(capacity, dtype=jnp.int32)

    experts = me ^ blocks[:minor]
    chosen = jnp.any(routing[None] == experts[:, None, None], axis=2)
    before = (blocks[None, :] < blocks[:, None])[None]
    rank = jnp.sum(before & chosen[:, None, :], axis=2)
    table = chosen[:, None, :] & (rank[:, None, :] == slots[None, :, None])
    hit = table[0].astype(jnp.int32)
    other = jnp.where(routing[:, 0] == me, routing[:, 1], routing[:, 0])
    home = jnp.sum(hit * blocks[None, :], axis=1)
    slot_task = jnp.sum(hit * task_ids[None, :], axis=1)
    slot_other = jnp.sum(hit * other[None, :], axis=1)
    spread = lambda x: jnp.broadcast_to(x.reshape(-1, 1), (x.size, LANES))

    source = spread((home ^ me).astype(jnp.float32))
    targets = me ^ (blocks[:major] * minor)
    place_mask = spread(
        jnp.any(
            table[None] & (blocks[None, None, None, :] == targets[:, None, None, None]), axis=3
        ).astype(jnp.bfloat16)
    )
    columns = jnp.arange(gate_weight.shape[1], dtype=jnp.int32)
    pick_self = columns[None, :] == (slot_task * n_experts + me)[:, None]
    pick_other = columns[None, :] == (slot_task * n_experts + slot_other)[:, None]
    pick = pick_self.astype(jnp.float32) - pick_other.astype(jnp.float32)

    weight_in, weight_out = w_in[0], w_out[0]

    def ffn(xs):
        return call(
            functools.partial(ffn_body, len(xs)),
            [shape(x.shape[0]) for x in xs],
            *xs, weight_in, weight_out,
            spare=16 * 2**20,
            flops=4 * sum(x.size for x in xs) * weight_in.shape[1],
        )

    edges = [sum(split[:i]) for i in range(len(split) + 1)]
    owns = [tokens[a:b] for a, b in zip(edges, edges[1:])]
    outs = []
    for stream, (own, rows) in enumerate(zip(owns, split)):
        full = shape(capacity * rows)

        gathered = {0: own}
        for mask in range(1, major):
            low = mask if stream in DIRECT else mask & -mask
            gathered[mask * minor] = move(gathered[(mask ^ low) * minor], low * minor)
        for ka in range(major):
            for kb in range(1, minor):
                gathered[ka * minor + kb] = move(gathered[ka * minor], kb)
        picked = call(
            functools.partial(select_body, capacity, n_experts),
            full,
            source, *[gathered[k] for k in range(n_experts)],
            flops=2e8,
            in_specs=[VMEM] + [ANY] * n_experts,
            scratch=[pltpu.SemaphoreType.DMA((capacity,))],
        )

        foreign = {chip: move_dp(picked, chip * CORES) for chip in range(1, chips)}
        near = move_dp(picked, 1)
        gate = call(
            functools.partial(gate_body, capacity),
            jax.ShapeDtypeStruct((capacity * rows, LANES), jnp.float32),
            pick, picked, gate_weight.T,
            flops=1e8,
        )
        mine, theirs = ffn([picked, near])
        theirs = move_dp(theirs, 1)
        backs = []
        for chip in range(1, chips):
            far = foreign[chip]
            far_near = move_dp(far, 1)
            (kept,) = ffn([far])
            (sent,) = ffn([far_near])
            sent = move_dp(sent, 1)
            summed = call(add_body, full, kept, sent, flops=1e8)
            backs.append(move_dp(summed, chip * CORES))
        gated = call(combine_body, full, gate, mine, theirs, *backs, flops=1e8)

        arrived = [gated] + [move(gated, kb) for kb in range(1, minor)]
        values = call(
            functools.partial(place_body, capacity, major, minor),
            [shape(rows)] * major,
            place_mask, *arrived,
            flops=1e8,
        )
        result = values[0].astype(jnp.float32)
        for mask in reversed(range(1, major)):
            result = result + move(values[mask], mask * minor).astype(jnp.float32)
        outs.append(result.astype(jnp.bfloat16))
    return jnp.concatenate(outs, axis=0)


def solution(mesh):
    placed = (
        P(("dp", "expert"), None),
        P("dp"),
        P("dp", None),
        P(),
        P("expert", None, "dp"),
        P("expert", "dp", None),
    )
    return jax.shard_map(
        shards, mesh=mesh, in_specs=placed, out_specs=P(("dp", "expert"), None), check_vma=False
    )
```
